32 devices in a mesh: rep: 4 (over x, core), grp: 8 (over z, y).
Axes of the slice: x: 2, y: 2, z: 4, core: 2. Of those that a mesh axis runs over, the one named last changes fastest.
Arguments:
- tokens: bfloat16 [8192, 2304], P(('rep', 'grp')), may hold values from -6 to 6
- norm_gain: float32 [2304], replicated, may hold values from 0.25 to 1.75
- key_weight: bfloat16 [2304, 1024], P('grp'), may hold values from -0.125 to 0.125
- key_grad: bfloat16 [8192, 1024], P(('rep', 'grp')), may hold values from -6 to 6
Outputs:
- token_grad: bfloat16 [8192, 2304], P(('rep', 'grp'))
- weight_grad: float32 [2304, 1024], P('grp', 'rep')
- gain_grad: float32 [2304], replicated
The draws below stay inside these ranges and needn't reach their ends.
All inputs are finite; a program needn't handle non-finite values.
Results may differ from the reference program's by a relative error of at most 0.023.
Values may be sent and summed in bfloat16 or wider, within the bound.
No kernel may reach another device: no remote copies, remote signals or barrier semaphores. Data moves between devices by JAX's collectives and lax.ppermute only.
A program may use at most 64 MiB of HBM per device.

```python
import jax
import jax.numpy as jnp
from jax import lax

D = 2304
KV_HEADS = 8
HEAD_DIM = 128
KEYS = 1024
TOK_DEV = 256
TOKENS = 8192
N_REP = 4
N_GRP = 8


def block_levels(key, extent, pieces, low, largest):
    def one(axis_at, blocks):
        steps = jax.random.uniform(jax.random.fold_in(jax.random.fold_in(key, 6), axis_at), (blocks,), jnp.float32, low / len(pieces), largest / len(pieces))
        return jnp.repeat(jnp.exp(steps), extent[axis_at] // blocks).reshape((-1,) + (1,) * (len(extent) - axis_at - 1))

    loudness = one(*pieces[0])
    for cut in pieces[1:]:
        loudness = loudness * one(*cut)
    return loudness


def bell_draw(own_key, dims, spread, reach, shards=(), dtype=jnp.bfloat16):
    array = jax.random.normal(own_key, dims, jnp.float32) * spread
    if len(shards) > 0:
        array = block_levels(own_key, dims, shards, -0.22, 0.18) * array
    return jnp.clip(array, min=-reach, max=reach).astype(dtype)


def setup_inputs(seed: int = 0) -> dict:
    key_list = jax.random.split(jax.random.key(seed), 5)
    tokens = bell_draw(key_list[0], (TOKENS, D), 1.0, 6.0, ((0, 32),))
    norm_gain = jnp.clip(1.0 + 0.15 * jax.random.normal(key_list[1], (D,), jnp.float32), 0.25, 1.75)
    key_weight = bell_draw(key_list[2], (D, KEYS), D ** -0.5, 0.125, ((0, 8),))
    key_grad = bell_draw(key_list[3], (TOKENS, KEYS), 1.0, 6.0, ((0, 32),))
    return {"tokens": tokens, "norm_gain": norm_gain, "key_weight": key_weight, "key_grad": key_grad}


epsilon = 1e-06

def reference(tokens, norm_gain, key_weight, key_grad):
    grad_scale = (TOK_DEV * N_REP * N_GRP) ** (-0.5)
    blocks = tokens.reshape(N_REP * N_GRP, TOK_DEV, D)
    key_blocks = key_grad.reshape(N_REP * N_GRP, TOK_DEV, KV_HEADS * HEAD_DIM)

    def one_block(carry, inputs):
        running, gain_total = carry
        block_tokens, block_keys = inputs
        wide_tokens = block_tokens.astype(jnp.float32)
        inv_rms = lax.rsqrt(lax.optimization_barrier(jnp.mean(wide_tokens * wide_tokens, axis=1, keepdims=True)) + epsilon)
        normed = (wide_tokens * inv_rms * norm_gain).astype(jnp.bfloat16)
        partial_value = lax.dot_general(normed, block_keys, (((0,), (0,)), ((), ())), preferred_element_type=jnp.float32)
        rounded = lax.optimization_barrier(partial_value.astype(jnp.bfloat16)).astype(jnp.float32)
        d_normed = lax.dot_general(block_keys, key_weight, (((1,), (1,)), ((), ())), preferred_element_type=jnp.float32)
        gain_part = lax.optimization_barrier(jnp.sum(d_normed * wide_tokens * inv_rms, axis=0))
        scaled = d_normed * norm_gain
        inner_mean = lax.optimization_barrier(jnp.mean(scaled * wide_tokens, axis=1, keepdims=True))
        block_grad = (inv_rms * (scaled - wide_tokens * inv_rms * inv_rms * inner_mean)).astype(jnp.bfloat16)
        return ((running + rounded, gain_total + gain_part), block_grad)
    start = (jnp.zeros((D, KV_HEADS * HEAD_DIM), jnp.float32), jnp.zeros((D,), jnp.float32))
    (running, gain_total), grads = lax.scan(one_block, start, (blocks, key_blocks))
    token_grad = grads.reshape(N_REP * N_GRP * TOK_DEV, D)
    return (token_grad, running * grad_scale, gain_total * grad_scale)
```

```python
import jax
import jax.numpy as jnp
from jax import lax
from jax.sharding import PartitionSpec as P

epsilon = 1e-06


def swap(value, axis, flip):
    size = lax.axis_size(axis)
    return lax.ppermute(value, axis, [(i, i ^ flip) for i in range(size)])


def tree_sum(parts):
    while len(parts) > 1:
        parts = [parts[i] + parts[i + 1] for i in range(0, len(parts), 2)]
    return parts[0]


def sum_everywhere(value, axis):
    size = lax.axis_size(axis)
    step = 1
    while step < size:
        radix = min(8, size // step)
        value = tree_sum([value] + [swap(value, axis, step * k) for k in range(1, radix)])
        step *= radix
    return value


def shards(tokens, norm_gain, key_weight, key_grad):
    f32, bf16 = jnp.float32, jnp.bfloat16
    n_rep, n_grp = lax.axis_size("rep"), lax.axis_size("grp")
    rep, grp = lax.axis_index("rep"), lax.axis_index("grp")
    grad_scale = (tokens.shape[0] * n_rep * n_grp) ** (-0.5)
    features, keys = key_weight.shape[0] * n_grp, key_weight.shape[1]
    rows, cols, half = key_weight.shape[0], keys // n_rep, keys // 2
    core = rep % 2

    own = lax.dynamic_slice_in_dim(key_weight, core * half, half, 1)
    pieces = {0: own}
    for flip in range(2, n_grp, 2):
        pieces[flip] = swap(own, "grp", flip)
    for flip in range(0, n_grp, 2):
        pieces[flip + 1] = swap(pieces[flip], "grp", 1)

    wide_tokens = tokens.astype(f32)
    inv_rms = lax.rsqrt(jnp.mean(wide_tokens * wide_tokens, axis=1, keepdims=True) + epsilon)
    normed = (wide_tokens * inv_rms * norm_gain).astype(bf16)

    def partial(flip):
        block = lax.dynamic_slice_in_dim(key_grad, (rep ^ flip) * cols, cols, 1)
        return lax.dot_general(normed, block, (((0,), (0,)), ((), ())), preferred_element_type=f32)

    crossing = {}
    for flip in list(range(2, n_rep, 2)) + [0]:
        crossing[flip] = swap(partial(flip + 1).astype(bf16), "rep", 1)
    sent = {}
    for flip in range(2, n_rep, 2):
        sent[flip] = swap((partial(flip) + crossing[flip].astype(f32)).astype(bf16), "rep", flip)
    section = partial(0) + crossing[0].astype(f32)
    for flip in sent:
        section = section + sent[flip].astype(f32)
    narrow = section.astype(bf16)
    weight_sum = lax.dynamic_slice_in_dim(section, grp * rows, rows, 0)
    for flip in range(1, n_grp):
        block = lax.dynamic_slice_in_dim(narrow, (grp ^ flip) * rows, rows, 0)
        weight_sum = weight_sum + swap(block, "grp", flip).astype(f32)

    gathered = jnp.zeros((features, half), bf16)
    for flip in range(n_grp):
        gathered = lax.dynamic_update_slice_in_dim(gathered, pieces[flip], (grp ^ flip) * rows, 0)
    other = swap(gathered, "rep", 1)

    def back(weight, at):
        block = lax.dynamic_slice_in_dim(key_grad, at * half, half, 1)
        return lax.dot_general(block, weight, (((1,), (1,)), ((), ())), preferred_element_type=f32)

    d_normed = back(gathered, core) + back(other, 1 - core)
    gain_local = jnp.sum(d_normed * wide_tokens * inv_rms, axis=0)
    gain_total = sum_everywhere(sum_everywhere(gain_local, "rep"), "grp")
    scaled = d_normed * norm_gain
    inner_mean = jnp.mean(scaled * wide_tokens, axis=1, keepdims=True)
    token_grad = (inv_rms * (scaled - wide_tokens * inv_rms * inv_rms * inner_mean)).astype(bf16)
    return (token_grad, weight_sum * grad_scale, gain_total * grad_scale)


def solution(mesh):
    in_specs = (P(("rep", "grp"), None), P(), P("grp", None), P(("rep", "grp"), None))
    out_specs = (P(("rep", "grp"), None), P("grp", "rep"), P())
    return jax.shard_map(shards, mesh=mesh, in_specs=in_specs, out_specs=out_specs, check_vma=False)
```

```python
import jax
import jax.numpy as jnp
from jax import lax
from jax.sharding import PartitionSpec as P


epsilon = 1e-06


def swap(value, axis, flip):
    size = lax.axis_size(axis)
    return lax.ppermute(value, axis, [(i, i ^ flip) for i in range(size)])


def tree_sum(parts):
    while len(parts) > 1:
        parts = [parts[i] + parts[i + 1] for i in range(0, len(parts), 2)]
    return parts[0]


def sum_everywhere(value, axis):
    size = lax.axis_size(axis)
    step = 1
    while step < size:
        radix = min(8, size // step)
        value = tree_sum([value] + [swap(value, axis, step * k) for k in range(1, radix)])
        step *= radix
    return value


def shards(tokens, norm_gain, key_weight, key_grad):
    f32, bf16 = jnp.float32, jnp.bfloat16
    n_rep, n_grp = lax.axis_size("rep"), lax.axis_size("grp")
    rep, grp = lax.axis_index("rep"), lax.axis_index("grp")
    grad_scale = (tokens.shape[0] * n_rep * n_grp) ** (-0.5)
    features, keys = key_weight.shape[0] * n_grp, key_weight.shape[1]
    rows, cols, half = key_weight.shape[0], keys // n_rep, keys // 2
    core = rep % 2

    own = lax.dynamic_slice_in_dim(key_weight, core * half, half, 1)
    pieces = {0: own}
    for flip in range(2, n_grp, 2):
        pieces[flip] = swap(own, "grp", flip)
    for flip in range(0, n_grp, 2):
        pieces[flip + 1] = swap(pieces[flip], "grp", 1)

    wide_tokens = tokens.astype(f32)
    inv_rms = lax.rsqrt(jnp.mean(wide_tokens * wide_tokens, axis=1, keepdims=True) + epsilon)
    normed = (wide_tokens * inv_rms * norm_gain).astype(bf16)

    def partial(flip):
        block = lax.dynamic_slice_in_dim(key_grad, (rep ^ flip) * cols, cols, 1)
        return lax.dot_general(normed, block, (((0,), (0,)), ((), ())), preferred_element_type=f32)

    crossing = {}
    for flip in list(range(2, n_rep, 2)) + [0]:
        crossing[flip] = swap(partial(flip + 1).astype(bf16), "rep", 1)
    sent = {}
    for flip in range(2, n_rep, 2):
        sent[flip] = swap((partial(flip) + crossing[flip].astype(f32)).astype(bf16), "rep", flip)
    section = partial(0) + crossing[0].astype(f32)
    for flip in sent:
        section = section + sent[flip].astype(f32)
    narrow = section.astype(bf16)
    weight_sum = lax.dynamic_slice_in_dim(section, grp * rows, rows, 0)
    arriving = []
    for flip in range(1, n_grp):
        block = lax.dynamic_slice_in_dim(narrow, (grp ^ flip) * rows, rows, 0)
        arriving.append(swap(block, "grp", flip))

    gathered = jnp.zeros((features, half), bf16)
    for flip in range(n_grp):
        gathered = lax.dynamic_update_slice_in_dim(gathered, pieces[flip], (grp ^ flip) * rows, 0)
    other = swap(gathered, "rep", 1)

    def back(weight, at):
        block = lax.dynamic_slice_in_dim(key_grad, at * half, half, 1)
        return lax.dot_general(block, weight, (((1,), (1,)), ((), ())), preferred_element_type=f32)

    d_normed = back(gathered, core) + back(other, 1 - core)
    gain_local = jnp.sum(d_normed * wide_tokens * inv_rms, axis=0)
    gain_total = sum_everywhere(sum_everywhere(gain_local, "rep"), "grp")
    scaled = d_normed * norm_gain
    inner_mean = jnp.mean(scaled * wide_tokens, axis=1, keepdims=True)
    token_grad = (inv_rms * (scaled - wide_tokens * inv_rms * inv_rms * inner_mean)).astype(bf16)
    arriving, token_grad, gain_total = lax.optimization_barrier((arriving, token_grad, gain_total))
    for block in arriving:
        weight_sum = weight_sum + block.astype(f32)
    return (token_grad, weight_sum * grad_scale, gain_total * grad_scale)


def solution(mesh):
    in_specs = (P(("rep", "grp"), None), P(), P("grp", None), P(("rep", "grp"), None))
    out_specs = (P(("rep", "grp"), None), P("grp", "rep"), P())
    return jax.shard_map(shards, mesh=mesh, in_specs=in_specs, out_specs=out_specs, check_vma=False)
```

```python
import jax
import jax.numpy as jnp
from jax import lax
from jax.sharding import PartitionSpec as P


epsilon = 1e-06


def swap(value, axis, flip):
    size = lax.axis_size(axis)
    return lax.ppermute(value, axis, [(i, i ^ flip) for i in range(size)])


def tree_sum(parts):
    while len(parts) > 1:
        parts = [parts[i] + parts[i + 1] for i in range(0, len(parts), 2)]
    return parts[0]


def sum_everywhere(value, axis):
    size = lax.axis_size(axis)
    step = 1
    while step < size:
        radix = min(8, size // step)
        value = tree_sum([value] + [swap(value, axis, step * k) for k in range(1, radix)])
        step *= radix
    return value


def shards(tokens, norm_gain, key_weight, key_grad):
    f32, bf16 = jnp.float32, jnp.bfloat16
    n_rep, n_grp = lax.axis_size("rep"), lax.axis_size("grp")
    rep, grp = lax.axis_index("rep"), lax.axis_index("grp")
    grad_scale = (tokens.shape[0] * n_rep * n_grp) ** (-0.5)
    rows, keys = key_weight.shape
    cols, half = keys // n_rep, keys // 2
    core = rep % 2

    own = lax.dynamic_slice_in_dim(key_weight, core * half, half, 1)
    pieces = {0: own, 1: swap(own, "grp", 1)}
    for flip in range(2, n_grp, 2):
        if flip == 2 or flip % 4 == 0:
            pieces[flip] = swap(own, "grp", flip)
    for flip in range(6, n_grp, 4):
        pieces[flip] = swap(pieces[flip - 2], "grp", 2)
    for flip in range(2, n_grp, 2):
        pieces[flip + 1] = swap(pieces[flip], "grp", 1)

    wide_tokens = tokens.astype(f32)
    inv_rms = lax.rsqrt(jnp.mean(wide_tokens * wide_tokens, axis=1, keepdims=True) + epsilon)
    normed = (wide_tokens * inv_rms * norm_gain).astype(bf16)

    def partial(flip):
        block = lax.dynamic_slice_in_dim(key_grad, (rep ^ flip) * cols, cols, 1)
        return lax.dot_general(normed, block, (((0,), (0,)), ((), ())), preferred_element_type=f32)

    crossing = {}
    for flip in list(range(2, n_rep, 2)) + [0]:
        crossing[flip] = swap(partial(flip + 1).astype(bf16), "rep", 1)
    sent = {}
    for flip in range(2, n_rep, 2):
        sent[flip] = swap((partial(flip) + crossing[flip].astype(f32)).astype(bf16), "rep", flip)
    section = partial(0) + crossing[0].astype(f32)
    for flip in sent:
        section = section + sent[flip].astype(f32)
    narrow = section.astype(bf16)
    weight_sum = lax.dynamic_slice_in_dim(section, grp * rows, rows, 0)
    arriving = []
    for flip in range(1, n_grp):
        block = lax.dynamic_slice_in_dim(narrow, (grp ^ flip) * rows, rows, 0)
        arriving.append(swap(block, "grp", flip))

    canvas, pieces[1] = lax.optimization_barrier((own, pieces[1]))
    gathered = jnp.tile(canvas, (n_grp, 1))
    for flip in range(1, n_grp):
        gathered = lax.dynamic_update_slice_in_dim(gathered, pieces[flip], (grp ^ flip) * rows, 0)
    other = swap(gathered, "rep", 1)

    def back(weight, at):
        block = lax.dynamic_slice_in_dim(key_grad, at * half, half, 1)
        return lax.dot_general(block, weight, (((1,), (1,)), ((), ())), preferred_element_type=f32)

    d_normed = back(gathered, core) + back(other, 1 - core)
    gain_local = jnp.sum(d_normed * wide_tokens * inv_rms, axis=0)
    gain_total = sum_everywhere(sum_everywhere(gain_local, "rep"), "grp")
    scaled = d_normed * norm_gain
    inner_mean = jnp.mean(scaled * wide_tokens, axis=1, keepdims=True)
    token_grad = (inv_rms * (scaled - wide_tokens * inv_rms * inv_rms * inner_mean)).astype(bf16)
    arriving, token_grad, gain_total = lax.optimization_barrier((arriving, token_grad, gain_total))
    for block in arriving:
        weight_sum = weight_sum + block.astype(f32)
    return (token_grad, weight_sum * grad_scale, gain_total * grad_scale)


def solution(mesh):
    in_specs = (P(("rep", "grp"), None), P(), P("grp", None), P(("rep", "grp"), None))
    out_specs = (P(("rep", "grp"), None), P("grp", "rep"), P())
    return jax.shard_map(shards, mesh=mesh, in_specs=in_specs, out_specs=out_specs, check_vma=False)
```

```python
import jax
import jax.numpy as jnp
from jax import lax
from jax.sharding import PartitionSpec as P


epsilon = 1e-06


def swap(value, axis, flip):
    size = lax.axis_size(axis)
    return lax.ppermute(value, axis, [(i, i ^ flip) for i in range(size)])


def tree_sum(parts):
    while len(parts) > 1:
        parts = [parts[i] + parts[i + 1] for i in range(0, len(parts), 2)]
    return parts[0]


def sum_everywhere(value, axis):
    size = lax.axis_size(axis)
    step = 1
    while step < size:
        radix = min(8, size // step)
        value = tree_sum([value] + [swap(value, axis, step * k) for k in range(1, radix)])
        step *= radix
    return value


def shards(tokens, norm_gain, key_weight, key_grad):
    f32, bf16 = jnp.float32, jnp.bfloat16
    n_rep, n_grp = lax.axis_size("rep"), lax.axis_size("grp")
    rep, grp = lax.axis_index("rep"), lax.axis_index("grp")
    grad_scale = (tokens.shape[0] * n_rep * n_grp) ** (-0.5)
    rows, keys = key_weight.shape
    cols, half = keys // n_rep, keys // 2
    core = rep % 2

    own = lax.dynamic_slice_in_dim(key_weight, core * half, half, 1)
    pieces = {0: own, 1: swap(own, "grp", 1)}
    for flip in range(2, n_grp, 2):
        if flip == 2 or flip % 4 == 0:
            pieces[flip] = swap(own, "grp", flip)
    for flip in range(6, n_grp, 4):
        pieces[flip] = swap(pieces[flip - 2], "grp", 2)
    for flip in range(2, n_grp, 2):
        pieces[flip + 1] = swap(pieces[flip], "grp", 1)

    wide_tokens = tokens.astype(f32)
    inv_rms = lax.rsqrt(jnp.mean(wide_tokens * wide_tokens, axis=1, keepdims=True) + epsilon)
    normed = (wide_tokens * inv_rms * norm_gain).astype(bf16)

    def partial(flip):
        block = lax.dynamic_slice_in_dim(key_grad, (rep ^ flip) * cols, cols, 1)
        return lax.dot_general(normed, block, (((0,), (0,)), ((), ())), preferred_element_type=f32)

    crossing = {}
    for flip in list(range(2, n_rep, 2)) + [0]:
        crossing[flip] = swap(partial(flip + 1).astype(bf16), "rep", 1)

    def side(value, flip):
        blocks = value.reshape(n_grp // 2, 2, rows, cols)
        return lax.dynamic_index_in_dim(blocks, (grp % 2) ^ flip, 1, keepdims=False)

    sent = {0: [], 1: []}
    for flip in range(2, n_rep, 2):
        summed = (partial(flip) + crossing[flip].astype(f32)).astype(bf16)
        sent[1].append(swap(side(summed, 1), "rep", flip))
        sent[0].append(swap(side(summed, 0), "rep", flip))
    local = partial(0) + crossing[0].astype(f32)
    sections, narrow = {}, {}
    for y_flip in (1, 0):
        if y_flip == 0 and sent[0]:
            sent[0][0], _ = lax.optimization_barrier((sent[0][0], narrow[1]))
        sections[y_flip] = side(local, y_flip)
        for block in sent[y_flip]:
            sections[y_flip] = sections[y_flip] + block.astype(f32)
        narrow[y_flip] = sections[y_flip].astype(bf16)
    pieces[n_grp - 1], _ = lax.optimization_barrier((pieces[n_grp - 1], narrow[1]))
    weight_sum = lax.dynamic_index_in_dim(sections[0], grp // 2, 0, keepdims=False)
    arriving = []
    for flip in list(range(1, n_grp, 2)) + list(range(2, n_grp, 2)):
        block = lax.dynamic_index_in_dim(narrow[flip % 2], (grp ^ flip) // 2, 0, keepdims=False)
        arriving.append(swap(block, "grp", flip))

    canvas, pieces[1] = lax.optimization_barrier((own, pieces[1]))
    gathered = jnp.tile(canvas, (n_grp, 1))
    for flip in range(1, n_grp):
        gathered = lax.dynamic_update_slice_in_dim(gathered, pieces[flip], (grp ^ flip) * rows, 0)
    other = swap(gathered, "rep", 1)

    def back(weight, at):
        block = lax.dynamic_slice_in_dim(key_grad, at * half, half, 1)
        return lax.dot_general(block, weight, (((1,), (1,)), ((), ())), preferred_element_type=f32)

    d_normed = back(gathered, core) + back(other, 1 - core)
    gain_local = jnp.sum(d_normed * wide_tokens * inv_rms, axis=0)
    gain_total = sum_everywhere(sum_everywhere(gain_local, "rep"), "grp")
    scaled = d_normed * norm_gain
    inner_mean = jnp.mean(scaled * wide_tokens, axis=1, keepdims=True)
    token_grad = (inv_rms * (scaled - wide_tokens * inv_rms * inv_rms * inner_mean)).astype(bf16)
    arriving, token_grad, gain_total = lax.optimization_barrier((arriving, token_grad, gain_total))
    for block in arriving:
        weight_sum = weight_sum + block.astype(f32)
    return (token_grad, weight_sum * grad_scale, gain_total * grad_scale)


def solution(mesh):
    in_specs = (P(("rep", "grp"), None), P(), P("grp", None), P(("rep", "grp"), None))
    out_specs = (P(("rep", "grp"), None), P("grp", "rep"), P())
    return jax.shard_map(shards, mesh=mesh, in_specs=in_specs, out_specs=out_specs, check_vma=False)
```
